32 devices in a mesh: parts: 2 (over x), dp: 16 (over z, y, core).
Axes of the slice: x: 2, y: 2, z: 4, core: 2. Of those that a mesh axis runs over, the one named last changes fastest.
Arguments:
- activations: bfloat16 [8192, 14336], P(('parts', 'dp')), parts along dimension 0, may hold values from -6 to 6
- out_grads: bfloat16 [8192, 4096], P(('parts', 'dp')), parts along dimension 0, may hold values from -6 to 6
- lengths: int32 [32, 4], P(('parts', 'dp')), parts along dimension 0, may hold values from 1 to 128, 256 in all within a row
- proj_in: bfloat16 [14336, 64], replicated, may hold values from -0.046875 to 0.046875
- proj_out: bfloat16 [4096, 64], replicated, may hold values from -0.09375 to 0.09375
- queries: bfloat16 [1024, 4096], P(('parts', 'dp')), parts along dimension 0, may hold values from -0.01171875 to 0.01171875
Outputs:
- scores: bfloat16 [128, 512], P(('parts', 'dp')), parts along dimension 0
The draws below stay inside these ranges and needn't reach their ends.
There are 2 independent parts, one for each index of `parts`. The reference program is written for one: setup_inputs(seed, part) draws one part's arguments, and reference() takes and returns one part's arrays. A program takes and returns all parts, laid end to end along the dimension named above; an argument that names none is the same for every part. Nothing has to cross between parts.
Inputs may be any that keep to these rules, and one draw needn't show every extreme that they name: Each row of lengths sums to 256, and one entry of each row equals 128.
All inputs are finite; a program needn't handle non-finite values.
Results may differ from the reference program's by a relative error of at most 0.0065.
Values may be sent and summed in bfloat16 or wider, within the bound.
A program may use at most 128 MiB of HBM per device.

```python
import math
import jax
import jax.numpy as jnp
import numpy as np

D = 4096
FF = 14336
RANK = 64
TOK_DEV = 256
EX_DEV = 4
TOKENS = 4096
N_TRAIN = 64
NQ = 512
PARAMS = 4096
MOST = 128
N_DP = 16


def level_of(rng, dims, pieces, smallest, top_value):
    level = 1.0
    for dim, shards_of in pieces:
        heights = jax.random.uniform(jax.random.fold_in(jax.random.fold_in(rng, 6), dim), (shards_of,), jnp.float32, smallest / len(pieces), top_value / len(pieces))
        level = level * jnp.repeat(jnp.exp(heights), dims[dim] // shards_of).reshape((-1,) + (1,) * (len(dims) - 1 - dim))
    return level


def split_up(number_of, total, reach, lean):
    weights = [(1 << 20) // math.isqrt(standing ** lean) + 1 for standing in range(2, number_of + 1)]
    surplus, holding = total - reach - (number_of - 1), [1] * (number_of - 1)
    while surplus > 0:
        free = [i for i in range(number_of - 1) if holding[i] < reach]
        mass, remaining = sum([weights[i] for i in free]), surplus
        for i in free:
            more = min(reach - holding[i], max(1, remaining * weights[i] // mass), surplus)
            holding[i] = holding[i] + more
            surplus = surplus - more
    return np.array([reach] + holding)


def uneven(own_key, count, total, reach, lean):
    if count == 2:
        one = jax.random.randint(own_key, (), max(1, total - reach), min(reach, total - 1) + 1)
        return jnp.stack([one, total - one])
    sizes = jnp.asarray(split_up(count, total, reach, lean), jnp.int32)
    twos = (count - 1) // 2
    giver, sink = sizes[1:1 + 2 * twos:2], sizes[2:2 + 2 * twos:2]
    room = jnp.minimum(giver - 1, reach - sink)
    shifted = jax.random.randint(jax.random.fold_in(own_key, 1), (twos,), 0, 1 << 20) % (room + 1)
    sizes = sizes.at[1:1 + 2 * twos:2].set(giver - shifted).at[2:2 + 2 * twos:2].set(sink + shifted)
    return sizes[jax.random.permutation(jax.random.fold_in(own_key, 2), count)]


def scatter_about(own_key, extent, spread, reach, pieces=(), kind=jnp.bfloat16):
    entries = spread * jax.random.normal(own_key, extent, jnp.float32)
    if pieces:
        entries = entries * level_of(own_key, extent, pieces, -0.22, 0.18)
    return jnp.clip(entries, -reach, reach).astype(kind)


def setup_inputs(seed: int = 0, part: int = 0) -> dict:
    key_of = jax.random.split(jax.random.key(seed), 7)
    part_keys = jax.random.split(jax.random.fold_in(key_of[6], part), 7)
    activations = scatter_about(part_keys[0], (TOKENS, FF), 1.0, 6.0, ((0, 16),))
    out_grads = scatter_about(part_keys[1], (TOKENS, D), 1.0, 6.0, ((0, 16),))
    lengths = jax.vmap(lambda own: uneven(own, EX_DEV, TOK_DEV, MOST, 2))(jax.random.split(part_keys[2], N_DP)).reshape((N_DP, EX_DEV)).astype(jnp.int32)
    proj_in = scatter_about(key_of[3], (FF, RANK), FF ** -0.5, 0.046875)
    proj_out = scatter_about(key_of[4], (D, RANK), D ** -0.5, 0.09375)
    queries = scatter_about(part_keys[5], (NQ, PARAMS), (0.125 / RANK), 0.01171875, ((0, 16),))
    return dict(activations=activations, out_grads=out_grads, lengths=lengths, proj_in=proj_in, proj_out=proj_out, queries=queries)


def reference(activations, out_grads, lengths, proj_in, proj_out, queries):
    proj_acts = jnp.dot(activations, proj_in, preferred_element_type=jnp.float32).astype(jnp.bfloat16)
    proj_grads = jnp.dot(out_grads, proj_out, preferred_element_type=jnp.float32).astype(jnp.bfloat16)
    acts_wide = proj_acts.astype(jnp.float32)
    grads_wide = proj_grads.astype(jnp.float32)
    outer_terms = (grads_wide[:, :, None] * acts_wide[:, None, :]).reshape(TOKENS, RANK * RANK)
    tok_ends = jnp.cumsum(lengths.reshape(-1)).astype(jnp.int32)
    position = jnp.arange(TOKENS, dtype=jnp.int32)
    example_ids = jnp.searchsorted(tok_ends, position, side="right").astype(jnp.int32)
    example_grads = jax.ops.segment_sum(outer_terms, example_ids, num_segments=N_TRAIN).astype(jnp.bfloat16)
    return jnp.dot(example_grads, queries.T, preferred_element_type=jnp.float32).astype(jnp.bfloat16)
```

```python
import functools

import jax
import jax.numpy as jnp
from jax import lax
from jax.experimental import pallas as pl
from jax.experimental.pallas import tpu as pltpu
from jax.sharding import PartitionSpec as P

MESH = pl.DeviceIdType.MESH
NT = (((1,), (1,)), ((), ()))
NN = (((1,), (0,)), ((), ()))
CHUNKS = 4
PIECES = 2
GROUP = 4


def kernel(
    n,
    lens,
    acts_hbm,
    grads_hbm,
    win_hbm,
    wout_hbm,
    q_hbm,
    out_ref,
    acts,
    grads,
    win,
    wout,
    qs,
    rows,
    masks,
    expand,
    acc,
    stage,
    result,
    local_sem,
    acts_sem,
    grads_sem,
    q_send,
    q_recv,
    row_send,
    row_recv,
    mask_send,
    mask_recv,
    res_send,
    res_recv,
):
    me = lax.axis_index("dp")
    n_groups = n // GROUP
    group, lane = me // GROUP, lax.rem(me, GROUP)
    n_half, _, per_half, chunk, width = rows.shape
    ex = stage.shape[1]
    rank = width // 2
    pairs = rank // 2
    half, slot = group // per_half, lax.rem(group, per_half)
    ff = acts.shape[1]
    piece = ff // PIECES

    def peer(t):
        return lax.rem(group + t, n_groups) * GROUP + lane

    buddy = me + 1 - 2 * lax.rem(me, 2)
    across = me + 2 - 4 * lax.rem(me // 2, 2)
    across_lane = lax.rem(across, GROUP)

    load_q = pltpu.make_async_copy(q_hbm, qs.at[lane], local_sem.at[0])
    load_q.start()
    load_wout = pltpu.make_async_copy(wout_hbm, wout, local_sem.at[1])
    load_win = pltpu.make_async_copy(win_hbm, win, local_sem.at[2])
    load_wout.start()
    load_win.start()
    load_grads, load_acts = [], []
    for c in range(CHUNKS):
        span = pl.ds(c * chunk, chunk)
        load = pltpu.make_async_copy(grads_hbm.at[span], grads.at[span], grads_sem.at[c])
        load.start()
        load_grads.append(load)
        for p in range(PIECES):
            cols = pl.ds(p * piece, piece)
            load = pltpu.make_async_copy(
                acts_hbm.at[span, cols], acts.at[span, cols], acts_sem.at[c, p]
            )
            load.start()
            load_acts.append(load)

    barrier = pltpu.get_barrier_semaphore()
    peers = [peer(t) for t in range(1, n_groups)]
    for other in peers + [buddy, across]:
        pl.semaphore_signal(barrier, inc=1, device_id={"dp": other}, device_id_type=MESH)

    row_id = lax.broadcasted_iota(jnp.int32, (8, width), 0) - slot * ex
    lane_id = lax.broadcasted_iota(jnp.int32, (8, width), 1) - slot * chunk
    inside = (lane_id >= 0) & (lane_id < chunk)
    for c in range(CHUNKS):
        token = lane_id + c * chunk
        start = jnp.int32(0)
        mask = jnp.zeros((8, width), jnp.float32)
        for e in range(ex):
            end = start + lens[0, e]
            hit = inside & (row_id == e) & (token >= start) & (token < end)
            mask = jnp.where(hit, 1.0, mask)
            start = end
        masks[group, c] = mask
    r_id = lax.broadcasted_iota(jnp.int32, (16 * pairs, width), 0)
    c_id = lax.broadcasted_iota(jnp.int32, (16 * pairs, width), 1)
    odd = (r_id >= 8 * pairs).astype(jnp.int32)
    source = 2 * ((r_id - odd * 8 * pairs) // 8) + odd
    expand[...] = jnp.where(source == c_id, 1.0, 0.0).astype(jnp.bfloat16)
    acc[...] = jnp.zeros_like(acc)

    pl.semaphore_wait(barrier, len(peers) + 2)

    load_q.wait()
    q_copies = []
    for i, other in enumerate((across, buddy)):
        copy = pltpu.make_async_remote_copy(
            src_ref=qs.at[lane],
            dst_ref=qs.at[lane],
            send_sem=q_send.at[i],
            recv_sem=q_recv.at[i],
            device_id={"dp": other},
            device_id_type=MESH,
        )
        copy.start()
        q_copies.append(copy)
    mask_copies = []
    for t in range(1, n_groups):
        copy = pltpu.make_async_remote_copy(
            src_ref=masks.at[group],
            dst_ref=masks.at[group],
            send_sem=mask_send.at[t - 1],
            recv_sem=mask_recv.at[t - 1],
            device_id={"dp": peer(t)},
            device_id_type=MESH,
        )
        copy.start()
        mask_copies.append(copy)

    load_wout.wait()
    load_win.wait()
    row_copies = []
    for c in range(CHUNKS):
        span = pl.ds(c * chunk, chunk)
        load_grads[c].wait()
        g = lax.dot_general(grads[span], wout[...], NT, preferred_element_type=jnp.float32)
        a = jnp.zeros((chunk, rank), jnp.float32)
        for p in range(PIECES):
            load_acts[c * PIECES + p].wait()
            cols = pl.ds(p * piece, piece)
            a = a + lax.dot_general(
                acts[span, cols], win[:, cols], NT, preferred_element_type=jnp.float32
            )
        rows[half, c, slot] = jnp.concatenate([g, a], axis=1).astype(jnp.bfloat16)
        copies = []
        for t in range(1, n_groups):
            copy = pltpu.make_async_remote_copy(
                src_ref=rows.at[half, c, slot],
                dst_ref=rows.at[half, c, slot],
                send_sem=row_send.at[t - 1, c],
                recv_sem=row_recv.at[t - 1, c],
                device_id={"dp": peer(t)},
                device_id_type=MESH,
            )
            copy.start()
            copies.append(copy)
        row_copies.append(copies)

    def gather(c):
        for copy in row_copies[c]:
            copy.wait_recv()
        for h in range(n_half):
            block = rows[h, c].reshape(per_half * chunk, width)
            mask = masks[h * per_half, c]
            for s in range(1, per_half):
                mask = mask + masks[h * per_half + s, c]
            wide = lax.dot_general(expand[...], block, NT, preferred_element_type=jnp.float32)
            wide = wide.reshape(2 * pairs, 8, width) * mask[None]
            wide = wide.reshape(16 * pairs, width).astype(jnp.bfloat16)
            acc[h] += lax.dot_general(wide, block, NN, preferred_element_type=jnp.float32)

    for copy in mask_copies:
        copy.wait_recv()
    gather(0)
    gather(1)
    q_copies[0].wait_recv()
    relay = pltpu.make_async_remote_copy(
        src_ref=qs.at[across_lane],
        dst_ref=qs.at[across_lane],
        send_sem=q_send.at[2],
        recv_sem=q_recv.at[2],
        device_id={"dp": buddy},
        device_id_type=MESH,
    )
    relay.start()
    for c in range(2, CHUNKS):
        gather(c)

    lower = lax.broadcasted_iota(jnp.int32, (8, width), 1) < rank
    columns = []
    for k in range(pairs):
        parts = []
        for h in range(n_half):
            even = pltpu.roll(acc[h, 8 * k : 8 * k + 8], rank, 1)
            odd_rows = acc[h, 8 * pairs + 8 * k : 8 * pairs + 8 * k + 8]
            parts.append(jnp.where(lower, even, odd_rows))
        columns.append(jnp.concatenate(parts, axis=0).astype(jnp.bfloat16))
    example_grads = jnp.concatenate(columns, axis=1)
    q_copies[1].wait_recv()
    relay.wait_recv()
    queries = qs[...].reshape(qs.shape[0] * qs.shape[1], qs.shape[2])
    scores = lax.dot_general(example_grads, queries, NT, preferred_element_type=jnp.float32)
    for s in range(n_groups):
        stage[s] = scores[s * ex : (s + 1) * ex].astype(jnp.bfloat16)
    res_copies = []
    for t in range(1, n_groups):
        copy = pltpu.make_async_remote_copy(
            src_ref=stage.at[lax.rem(group + t, n_groups)],
            dst_ref=result.at[group],
            send_sem=res_send.at[t - 1],
            recv_sem=res_recv.at[t - 1],
            device_id={"dp": peer(t)},
            device_id_type=MESH,
        )
        copy.start()
        res_copies.append(copy)
    result[group] = stage[group]
    for copy in res_copies:
        copy.wait_recv()
    cols = qs.shape[0] * qs.shape[1]
    for s in range(n_groups):
        out_ref[:, s * cols : (s + 1) * cols] = result[s]
    for copy in q_copies + [relay] + mask_copies + res_copies:
        copy.wait_send()
    for copies in row_copies:
        for copy in copies:
            copy.wait_send()


def local(n, activations, out_grads, lengths, proj_in, proj_out, queries):
    tokens, ff = activations.shape
    d = out_grads.shape[1]
    rank = proj_in.shape[1]
    ex = lengths.shape[1]
    nq, params = queries.shape
    n_groups = n // GROUP
    per_half = 8 // ex
    n_half = n_groups // per_half
    chunk = tokens // CHUNKS
    width = 2 * rank
    bf16, f32 = jnp.bfloat16, jnp.float32
    dma = pltpu.SemaphoreType.DMA
    others = n_groups - 1
    hbm = pl.BlockSpec(memory_space=pltpu.MemorySpace.HBM)
    return pl.pallas_call(
        functools.partial(kernel, n),
        out_shape=jax.ShapeDtypeStruct((ex, nq * n), bf16),
        in_specs=[pl.BlockSpec(memory_space=pltpu.MemorySpace.SMEM)] + [hbm] * 5,
        out_specs=pl.BlockSpec(memory_space=pltpu.MemorySpace.VMEM),
        scratch_shapes=[
            pltpu.VMEM((tokens, ff), bf16),
            pltpu.VMEM((tokens, d), bf16),
            pltpu.VMEM((rank, ff), bf16),
            pltpu.VMEM((rank, d), bf16),
            pltpu.VMEM((GROUP, nq, params), bf16),
            pltpu.VMEM((n_half, CHUNKS, per_half, chunk, width), bf16),
            pltpu.VMEM((n_groups, CHUNKS, 8, width), f32),
            pltpu.VMEM((8 * rank, width), bf16),
            pltpu.VMEM((n_half, 8 * rank, width), f32),
            pltpu.VMEM((n_groups, ex, GROUP * nq), bf16),
            pltpu.VMEM((n_groups, ex, GROUP * nq), bf16),
            dma((3,)),
            dma((CHUNKS, PIECES)),
            dma((CHUNKS,)),
            dma((3,)),
            dma((3,)),
            dma((others, CHUNKS)),
            dma((others, CHUNKS)),
            dma((others,)),
            dma((others,)),
            dma((others,)),
            dma((others,)),
        ],
        compiler_params=pltpu.CompilerParams(
            collective_id=0, has_side_effects=True, vmem_limit_bytes=60 * 1024 * 1024
        ),
    )(lengths, activations, out_grads, proj_in.T, proj_out.T, queries)


def solution(mesh):
    in_specs = (
        P(("parts", "dp"), None),
        P(("parts", "dp"), None),
        P(("parts", "dp"), None),
        P(),
        P(),
        P(("parts", "dp"), None),
    )
    out_specs = P(("parts", "dp"), None)
    body = functools.partial(local, mesh.shape["dp"])
    return jax.shard_map(body, mesh=mesh, in_specs=in_specs, out_specs=out_specs, check_vma=False)
```

```python
import functools

import jax
import jax.numpy as jnp
from jax import lax
from jax.experimental import pallas as pl
from jax.experimental.pallas import tpu as pltpu
from jax.sharding import PartitionSpec as P

MESH = pl.DeviceIdType.MESH
NT = (((1,), (1,)), ((), ()))
NN = (((1,), (0,)), ((), ()))
CHUNKS = (4, 8, 4)
PIECES = 4
GROUP = 4


def kernel(
    n,
    lens_hbm,
    acts_hbm,
    grads_hbm,
    win_hbm,
    wout_hbm,
    q_hbm,
    out_hbm,
    lens,
    acts,
    grads,
    win,
    wout,
    qs,
    expand,
    acc,
    stage,
    result,
    out_vmem,
    local_sem,
    acts_sem,
    grads_sem,
    win_sem,
    q_send,
    q_recv,
    row_send,
    row_recv,
    mask_send,
    mask_recv,
    res_send,
    res_recv,
    *per_chunk,
):
    count = len(per_chunk) // 2
    rows, masks = per_chunk[:count], per_chunk[count:]
    me = lax.axis_index("dp")
    n_groups = n // GROUP
    group, lane = me // GROUP, lax.rem(me, GROUP)
    n_half, per_half, _, width = rows[0].shape
    sizes = [ref.shape[2] for ref in rows]
    starts = [sum(sizes[:c]) for c in range(count)]
    ex = stage.shape[1]
    rank = width // 2
    pairs = rank // 2
    half, slot = group // per_half, lax.rem(group, per_half)
    ff = acts.shape[1]
    piece = ff // PIECES

    def peer(t):
        return lax.rem(group + t, n_groups) * GROUP + lane

    buddy = me + 1 - 2 * lax.rem(me, 2)
    across = me + 2 - 4 * lax.rem(me // 2, 2)
    across_lane = lax.rem(across, GROUP)

    def start(source, target, sem):
        load = pltpu.make_async_copy(source, target, sem)
        load.start()
        return load

    pieces = [pl.ds(p * piece, piece) for p in range(PIECES)]
    spans = [pl.ds(starts[c], sizes[c]) for c in range(count)]
    load_grads, load_acts = {}, {}

    def fetch_grads(c):
        span = spans[c]
        load_grads[c] = start(grads_hbm.at[span], grads.at[span], grads_sem.at[c])

    def fetch_acts(c, p):
        part = (spans[c], pieces[p])
        load_acts[c, p] = start(acts_hbm.at[*part], acts.at[*part], acts_sem.at[c, p])

    def fetch(c):
        if c < count:
            fetch_grads(c)
            for p in range(PIECES):
                fetch_acts(c, p)

    load_win = []
    for p in range(PIECES):
        part = win.at[:, pieces[p]]
        load_win.append(start(win_hbm.at[:, pieces[p]], part, win_sem.at[p]))
        fetch_acts(0, p)
    load_wout = start(wout_hbm, wout, local_sem.at[1])
    fetch_grads(0)
    load_lens = start(lens_hbm, lens, local_sem.at[3])
    load_q = start(q_hbm, qs.at[lane], local_sem.at[0])
    fetch(1)

    barrier = pltpu.get_barrier_semaphore()
    peers = [peer(t) for t in range(1, n_groups)]
    for other in peers + [buddy, across]:
        pl.semaphore_signal(barrier, inc=1, device_id={"dp": other}, device_id_type=MESH)

    row_copies = []
    for c in range(count):
        span = spans[c]
        total = jnp.zeros((rank, sizes[c]), jnp.float32)
        for p in range(PIECES):
            if c == 0:
                load_win[p].wait()
            load_acts[c, p].wait()
            if p == 0:
                fetch(c + 2)
            total = total + lax.dot_general(
                win[:, pieces[p]], acts[span, pieces[p]], NT, preferred_element_type=jnp.float32
            )
        if c == 0:
            load_wout.wait()
        load_grads[c].wait()
        other = lax.dot_general(wout[...], grads[span], NT, preferred_element_type=jnp.float32)
        both = jnp.concatenate([other, total], axis=0)
        rows[c][half, slot] = both.T.astype(jnp.bfloat16)
        if c == 0:
            load_lens.wait()
            for k in range(count):
                shape = masks[k].shape[1:]
                row_id = lax.broadcasted_iota(jnp.int32, shape, 0) - slot * ex
                lane_id = lax.broadcasted_iota(jnp.int32, shape, 1) - slot * sizes[k]
                inside = (lane_id >= 0) & (lane_id < sizes[k])
                token = lane_id + starts[k]
                first = jnp.int32(0)
                mask = jnp.zeros(shape, jnp.float32)
                for e in range(ex):
                    end = first + lens[0, e]
                    hit = inside & (row_id == e) & (token >= first) & (token < end)
                    mask = jnp.where(hit, 1.0, mask)
                    first = end
                masks[k][group] = mask
            r_id = lax.broadcasted_iota(jnp.int32, (16 * pairs, width), 0)
            c_id = lax.broadcasted_iota(jnp.int32, (16 * pairs, width), 1)
            odd = (r_id >= 8 * pairs).astype(jnp.int32)
            source = 2 * ((r_id - odd * 8 * pairs) // 8) + odd
            expand[...] = jnp.where(source == c_id, 1.0, 0.0).astype(jnp.bfloat16)
            acc[...] = jnp.zeros_like(acc)
            pl.semaphore_wait(barrier, len(peers) + 2)

            load_q.wait()
            q_copies = []
            for i, other in enumerate((across, buddy)):
                copy = pltpu.make_async_remote_copy(
                    src_ref=qs.at[lane],
                    dst_ref=qs.at[lane],
                    send_sem=q_send.at[i],
                    recv_sem=q_recv.at[i],
                    device_id={"dp": other},
                    device_id_type=MESH,
                )
                copy.start()
                q_copies.append(copy)
            mask_copies = []
            for k, t in [(k, t) for k in range(count) for t in range(1, n_groups)]:
                copy = pltpu.make_async_remote_copy(
                    src_ref=masks[k].at[group],
                    dst_ref=masks[k].at[group],
                    send_sem=mask_send.at[t - 1, k],
                    recv_sem=mask_recv.at[t - 1, k],
                    device_id={"dp": peer(t)},
                    device_id_type=MESH,
                )
                copy.start()
                mask_copies.append(copy)
        copies = []
        for t in range(1, n_groups):
            copy = pltpu.make_async_remote_copy(
                src_ref=rows[c].at[half, slot],
                dst_ref=rows[c].at[half, slot],
                send_sem=row_send.at[t - 1, c],
                recv_sem=row_recv.at[t - 1, c],
                device_id={"dp": peer(t)},
                device_id_type=MESH,
            )
            copy.start()
            copies.append(copy)
        row_copies.append(copies)

    def gather(c):
        for copy in row_copies[c]:
            copy.wait_recv()
        for h in range(n_half):
            block = rows[c][h].reshape(per_half * sizes[c], width)
            mask = masks[c][h * per_half]
            for s in range(1, per_half):
                mask = mask + masks[c][h * per_half + s]
            wide = lax.dot_general(expand[...], block, NT, preferred_element_type=jnp.float32)
            wide = wide.reshape(2 * pairs, 8, mask.shape[1]) * mask[None]
            wide = wide.reshape(16 * pairs, mask.shape[1]).astype(jnp.bfloat16)
            acc[h] += lax.dot_general(wide, block, NN, preferred_element_type=jnp.float32)

    for copy in mask_copies:
        copy.wait_recv()
    for c in range(count - 2):
        gather(c)
    q_copies[0].wait_recv()
    relay = pltpu.make_async_remote_copy(
        src_ref=qs.at[across_lane],
        dst_ref=qs.at[across_lane],
        send_sem=q_send.at[2],
        recv_sem=q_recv.at[2],
        device_id={"dp": buddy},
        device_id_type=MESH,
    )
    relay.start()
    for c in range(count - 2, count):
        gather(c)

    lower = lax.broadcasted_iota(jnp.int32, (8, width), 1) < rank
    columns = []
    for k in range(pairs):
        parts = []
        for h in range(n_half):
            even = pltpu.roll(acc[h, 8 * k : 8 * k + 8], rank, 1)
            odd_rows = acc[h, 8 * pairs + 8 * k : 8 * pairs + 8 * k + 8]
            parts.append(jnp.where(lower, even, odd_rows))
        columns.append(jnp.concatenate(parts, axis=0).astype(jnp.bfloat16))
    example_grads = jnp.concatenate(columns, axis=1)
    q_copies[1].wait_recv()
    relay.wait_recv()
    queries = qs[...].reshape(qs.shape[0] * qs.shape[1], qs.shape[2])
    scores = lax.dot_general(example_grads, queries, NT, preferred_element_type=jnp.float32)
    for s in range(n_groups):
        stage[s] = scores[s * ex : (s + 1) * ex].astype(jnp.bfloat16)
    res_copies = []
    for t in range(1, n_groups):
        copy = pltpu.make_async_remote_copy(
            src_ref=stage.at[lax.rem(group + t, n_groups)],
            dst_ref=result.at[group],
            send_sem=res_send.at[t - 1],
            recv_sem=res_recv.at[t - 1],
            device_id={"dp": peer(t)},
            device_id_type=MESH,
        )
        copy.start()
        res_copies.append(copy)
    result[group] = stage[group]
    for copy in res_copies:
        copy.wait_recv()
    cols = qs.shape[0] * qs.shape[1]
    for s in range(n_groups):
        out_vmem[:, s * cols : (s + 1) * cols] = result[s]
    store = pltpu.make_async_copy(out_vmem, out_hbm, local_sem.at[4])
    store.start()
    for copy in q_copies + [relay] + mask_copies + res_copies:
        copy.wait_send()
    for copies in row_copies:
        for copy in copies:
            copy.wait_send()
    store.wait()


def local(n, activations, out_grads, lengths, proj_in, proj_out, queries):
    tokens, ff = activations.shape
    d = out_grads.shape[1]
    rank = proj_in.shape[1]
    ex = lengths.shape[1]
    nq, params = queries.shape
    n_groups = n // GROUP
    per_half = 8 // ex
    n_half = n_groups // per_half
    sizes = [tokens * part // sum(CHUNKS) for part in CHUNKS]
    count = len(sizes)
    width = 2 * rank
    bf16, f32 = jnp.bfloat16, jnp.float32
    dma = pltpu.SemaphoreType.DMA
    others = n_groups - 1
    hbm = pl.BlockSpec(memory_space=pltpu.MemorySpace.HBM)
    return pl.pallas_call(
        functools.partial(kernel, n),
        out_shape=jax.ShapeDtypeStruct((ex, nq * n), bf16),
        in_specs=[hbm] * 6,
        out_specs=pl.BlockSpec(memory_space=pl.ANY),
        scratch_shapes=[
            pltpu.SMEM((1, ex), jnp.int32),
            pltpu.VMEM((tokens, ff), bf16),
            pltpu.VMEM((tokens, d), bf16),
            pltpu.VMEM((rank, ff), bf16),
            pltpu.VMEM((rank, d), bf16),
            pltpu.VMEM((GROUP, nq, params), bf16),
            pltpu.VMEM((8 * rank, width), bf16),
            pltpu.VMEM((n_half, 8 * rank, width), f32),
            pltpu.VMEM((n_groups, ex, GROUP * nq), bf16),
            pltpu.VMEM((n_groups, ex, GROUP * nq), bf16),
            pltpu.VMEM((ex, nq * n), bf16),
            dma((5,)),
            dma((count, PIECES)),
            dma((count,)),
            dma((PIECES,)),
            dma((3,)),
            dma((3,)),
            dma((others, count)),
            dma((others, count)),
            dma((others, count)),
            dma((others, count)),
            dma((others,)),
            dma((others,)),
        ]
        + [pltpu.VMEM((n_half, per_half, size, width), bf16) for size in sizes]
        + [pltpu.VMEM((n_groups, 8, per_half * size), f32) for size in sizes],
        compiler_params=pltpu.CompilerParams(
            collective_id=0, has_side_effects=True, vmem_limit_bytes=67000000
        ),
    )(lengths, activations, out_grads, proj_in.T, proj_out.T, queries)


def solution(mesh):
    in_specs = (
        P(("parts", "dp"), None),
        P(("parts", "dp"), None),
        P(("parts", "dp"), None),
        P(),
        P(),
        P(("parts", "dp"), None),
    )
    out_specs = P(("parts", "dp"), None)
    body = functools.partial(local, mesh.shape["dp"])
    return jax.shard_map(body, mesh=mesh, in_specs=in_specs, out_specs=out_specs, check_vma=False)
```

```python
import functools

import jax
import jax.numpy as jnp
from jax import lax
from jax.experimental import pallas as pl
from jax.experimental.pallas import tpu as pltpu
from jax.sharding import PartitionSpec as P

MESH = pl.DeviceIdType.MESH
NT = (((1,), (1,)), ((), ()))
NN = (((1,), (0,)), ((), ()))
CHUNKS = (4, 4, 4, 4)
PIECES = 4
GROUP = 4


def kernel(
    n,
    lens_hbm,
    acts_hbm,
    grads_hbm,
    win_hbm,
    wout_hbm,
    q_hbm,
    out_hbm,
    lens,
    acts,
    grads,
    win,
    wout,
    qs,
    expand,
    acc,
    stage,
    result,
    out_vmem,
    local_sem,
    acts_sem,
    grads_sem,
    win_sem,
    q_send,
    q_recv,
    row_send,
    row_recv,
    mask_send,
    mask_recv,
    res_send,
    res_recv,
    *per_chunk,
):
    count = len(per_chunk) // 2
    rows, masks = per_chunk[:count], per_chunk[count:]
    me = lax.axis_index("dp")
    n_groups = n // GROUP
    group, lane = me // GROUP, lax.rem(me, GROUP)
    n_half, per_half, _, width = rows[0].shape
    sizes = [ref.shape[2] for ref in rows]
    starts = [sum(sizes[:c]) for c in range(count)]
    ex = stage.shape[1]
    rank = width // 2
    pairs = rank // 2
    half, slot = group // per_half, lax.rem(group, per_half)
    ff = acts.shape[1]
    piece = ff // PIECES

    backward = (group < n_groups - group).astype(jnp.int32)

    def turn(t):
        return t + backward * (n_groups - 2 * t)

    def peer(t):
        t = turn(t)
        return lax.rem(group + t, n_groups) * GROUP + lane

    buddy = me + 1 - 2 * lax.rem(me, 2)
    across = me + 2 - 4 * lax.rem(me // 2, 2)
    across_lane = lax.rem(across, GROUP)

    def start(source, target, sem):
        load = pltpu.make_async_copy(source, target, sem)
        load.start()
        return load

    pieces = [pl.ds(p * piece, piece) for p in range(PIECES)]
    spans = [pl.ds(starts[c], sizes[c]) for c in range(count)]
    load_grads, load_acts = {}, {}

    def fetch_grads(c):
        span = spans[c]
        load_grads[c] = start(grads_hbm.at[span], grads.at[span], grads_sem.at[c])

    def fetch_acts(c, p):
        part = (spans[c], pieces[p])
        load_acts[c, p] = start(acts_hbm.at[*part], acts.at[*part], acts_sem.at[c, p])

    def fetch(c):
        if c < count:
            fetch_grads(c)
            for p in range(PIECES):
                fetch_acts(c, p)

    load_win = []
    for p in range(PIECES):
        part = win.at[:, pieces[p]]
        load_win.append(start(win_hbm.at[:, pieces[p]], part, win_sem.at[p]))
        fetch_acts(0, p)
    load_wout = start(wout_hbm, wout, local_sem.at[1])
    fetch_grads(0)
    load_lens = start(lens_hbm, lens, local_sem.at[3])
    load_q = start(q_hbm, qs.at[lane], local_sem.at[0])
    fetch(1)

    barrier = pltpu.get_barrier_semaphore()
    peers = [peer(t) for t in range(1, n_groups)]
    for other in peers + [buddy, across]:
        pl.semaphore_signal(barrier, inc=1, device_id={"dp": other}, device_id_type=MESH)

    row_copies = []
    for c in range(count):
        span = spans[c]
        total = jnp.zeros((rank, sizes[c]), jnp.float32)
        for p in range(PIECES):
            if c == 0:
                load_win[p].wait()
            load_acts[c, p].wait()
            if p == 0:
                fetch(c + 2)
            total = total + lax.dot_general(
                win[:, pieces[p]], acts[span, pieces[p]], NT, preferred_element_type=jnp.float32
            )
        if c == 0:
            load_wout.wait()
        load_grads[c].wait()
        other = lax.dot_general(wout[...], grads[span], NT, preferred_element_type=jnp.float32)
        both = jnp.concatenate([other, total], axis=0)
        rows[c][half, slot] = both.T.astype(jnp.bfloat16)
        if c == 0:
            load_lens.wait()
            for k in range(count):
                shape = masks[k].shape[1:]
                row_id = lax.broadcasted_iota(jnp.int32, shape, 0) - slot * ex
                lane_id = lax.broadcasted_iota(jnp.int32, shape, 1) - slot * sizes[k]
                inside = (lane_id >= 0) & (lane_id < sizes[k])
                token = lane_id + starts[k]
                first = jnp.int32(0)
                mask = jnp.zeros(shape, jnp.float32)
                for e in range(ex):
                    end = first + lens[0, e]
                    hit = inside & (row_id == e) & (token >= first) & (token < end)
                    mask = jnp.where(hit, 1.0, mask)
                    first = end
                masks[k][group] = mask
            r_id = lax.broadcasted_iota(jnp.int32, (16 * pairs, width), 0)
            c_id = lax.broadcasted_iota(jnp.int32, (16 * pairs, width), 1)
            odd = (r_id >= 8 * pairs).astype(jnp.int32)
            source = 2 * ((r_id - odd * 8 * pairs) // 8) + odd
            expand[...] = jnp.where(source == c_id, 1.0, 0.0).astype(jnp.bfloat16)
            acc[...] = jnp.zeros_like(acc)
            pl.semaphore_wait(barrier, len(peers) + 2)

            load_q.wait()
            q_copies = []
            for i, other in enumerate((across, buddy)):
                copy = pltpu.make_async_remote_copy(
                    src_ref=qs.at[lane],
                    dst_ref=qs.at[lane],
                    send_sem=q_send.at[i],
                    recv_sem=q_recv.at[i],
                    device_id={"dp": other},
                    device_id_type=MESH,
                )
                copy.start()
                q_copies.append(copy)
            mask_copies = []
            for k, t in [(k, t) for k in range(count) for t in range(1, n_groups)]:
                copy = pltpu.make_async_remote_copy(
                    src_ref=masks[k].at[group],
                    dst_ref=masks[k].at[group],
                    send_sem=mask_send.at[turn(t) - 1, k],
                    recv_sem=mask_recv.at[turn(t) - 1, k],
                    device_id={"dp": peer(t)},
                    device_id_type=MESH,
                )
                copy.start()
                mask_copies.append(copy)
        copies = []
        for t in range(1, n_groups):
            copy = pltpu.make_async_remote_copy(
                src_ref=rows[c].at[half, slot],
                dst_ref=rows[c].at[half, slot],
                send_sem=row_send.at[turn(t) - 1, c],
                recv_sem=row_recv.at[turn(t) - 1, c],
                device_id={"dp": peer(t)},
                device_id_type=MESH,
            )
            copy.start()
            copies.append(copy)
        row_copies.append(copies)

    def gather(c):
        for copy in row_copies[c]:
            copy.wait_recv()
        for h in range(n_half):
            block = rows[c][h].reshape(per_half * sizes[c], width)
            mask = masks[c][h * per_half]
            for s in range(1, per_half):
                mask = mask + masks[c][h * per_half + s]
            wide = lax.dot_general(expand[...], block, NT, preferred_element_type=jnp.float32)
            wide = wide.reshape(2 * pairs, 8, mask.shape[1]) * mask[None]
            wide = wide.reshape(16 * pairs, mask.shape[1]).astype(jnp.bfloat16)
            acc[h] += lax.dot_general(wide, block, NN, preferred_element_type=jnp.float32)

    for copy in mask_copies:
        copy.wait_recv()
    for c in range(count - 2):
        gather(c)
    q_copies[0].wait_recv()
    relay = pltpu.make_async_remote_copy(
        src_ref=qs.at[across_lane],
        dst_ref=qs.at[across_lane],
        send_sem=q_send.at[2],
        recv_sem=q_recv.at[2],
        device_id={"dp": buddy},
        device_id_type=MESH,
    )
    relay.start()
    for c in range(count - 2, count):
        gather(c)

    lower = lax.broadcasted_iota(jnp.int32, (8, width), 1) < rank
    columns = []
    for k in range(pairs):
        parts = []
        for h in range(n_half):
            even = pltpu.roll(acc[h, 8 * k : 8 * k + 8], rank, 1)
            odd_rows = acc[h, 8 * pairs + 8 * k : 8 * pairs + 8 * k + 8]
            parts.append(jnp.where(lower, even, odd_rows))
        columns.append(jnp.concatenate(parts, axis=0).astype(jnp.bfloat16))
    example_grads = jnp.concatenate(columns, axis=1)
    q_copies[1].wait_recv()
    relay.wait_recv()
    queries = qs[...].reshape(qs.shape[0] * qs.shape[1], qs.shape[2])
    scores = lax.dot_general(example_grads, queries, NT, preferred_element_type=jnp.float32)
    for s in range(n_groups):
        stage[s] = scores[s * ex : (s + 1) * ex].astype(jnp.bfloat16)
    res_copies = []
    for t in range(1, n_groups):
        copy = pltpu.make_async_remote_copy(
            src_ref=stage.at[lax.rem(group + turn(t), n_groups)],
            dst_ref=result.at[group],
            send_sem=res_send.at[turn(t) - 1],
            recv_sem=res_recv.at[turn(t) - 1],
            device_id={"dp": peer(t)},
            device_id_type=MESH,
        )
        copy.start()
        res_copies.append(copy)
    result[group] = stage[group]
    for copy in res_copies:
        copy.wait_recv()
    cols = qs.shape[0] * qs.shape[1]
    for s in range(n_groups):
        out_vmem[:, s * cols : (s + 1) * cols] = result[s]
    store = pltpu.make_async_copy(out_vmem, out_hbm, local_sem.at[4])
    store.start()
    for copy in q_copies + [relay] + mask_copies + res_copies:
        copy.wait_send()
    for copies in row_copies:
        for copy in copies:
            copy.wait_send()
    store.wait()


def local(n, activations, out_grads, lengths, proj_in, proj_out, queries):
    tokens, ff = activations.shape
    d = out_grads.shape[1]
    rank = proj_in.shape[1]
    ex = lengths.shape[1]
    nq, params = queries.shape
    n_groups = n // GROUP
    per_half = 8 // ex
    n_half = n_groups // per_half
    sizes = [tokens * part // sum(CHUNKS) for part in CHUNKS]
    count = len(sizes)
    width = 2 * rank
    bf16, f32 = jnp.bfloat16, jnp.float32
    dma = pltpu.SemaphoreType.DMA
    others = n_groups - 1
    hbm = pl.BlockSpec(memory_space=pltpu.MemorySpace.HBM)
    return pl.pallas_call(
        functools.partial(kernel, n),
        out_shape=jax.ShapeDtypeStruct((ex, nq * n), bf16),
        in_specs=[hbm] * 6,
        out_specs=pl.BlockSpec(memory_space=pl.ANY),
        scratch_shapes=[
            pltpu.SMEM((1, ex), jnp.int32),
            pltpu.VMEM((tokens, ff), bf16),
            pltpu.VMEM((tokens, d), bf16),
            pltpu.VMEM((rank, ff), bf16),
            pltpu.VMEM((rank, d), bf16),
            pltpu.VMEM((GROUP, nq, params), bf16),
            pltpu.VMEM((8 * rank, width), bf16),
            pltpu.VMEM((n_half, 8 * rank, width), f32),
            pltpu.VMEM((n_groups, ex, GROUP * nq), bf16),
            pltpu.VMEM((n_groups, ex, GROUP * nq), bf16),
            pltpu.VMEM((ex, nq * n), bf16),
            dma((5,)),
            dma((count, PIECES)),
            dma((count,)),
            dma((PIECES,)),
            dma((3,)),
            dma((3,)),
            dma((others, count)),
            dma((others, count)),
            dma((others, count)),
            dma((others, count)),
            dma((others,)),
            dma((others,)),
        ]
        + [pltpu.VMEM((n_half, per_half, size, width), bf16) for size in sizes]
        + [pltpu.VMEM((n_groups, 8, per_half * size), f32) for size in sizes],
        compiler_params=pltpu.CompilerParams(
            collective_id=0, has_side_effects=True, vmem_limit_bytes=56500000
        ),
    )(pltpu.with_memory_space_constraint(lengths, pltpu.HBM), activations, out_grads, proj_in.T, proj_out.T, queries)


def solution(mesh):
    in_specs = (
        P(("parts", "dp"), None),
        P(("parts", "dp"), None),
        P(("parts", "dp"), None),
        P(),
        P(),
        P(("parts", "dp"), None),
    )
    out_specs = P(("parts", "dp"), None)
    body = functools.partial(local, mesh.shape["dp"])
    return jax.shard_map(body, mesh=mesh, in_specs=in_specs, out_specs=out_specs, check_vma=False)
```

```python
import functools

import jax
import jax.numpy as jnp
from jax import lax
from jax.experimental import pallas as pl
from jax.experimental.pallas import tpu as pltpu
from jax.sharding import PartitionSpec as P

MESH = pl.DeviceIdType.MESH
NT = (((1,), (1,)), ((), ()))
NN = (((1,), (0,)), ((), ()))
CHUNKS = (4, 4, 5, 3)
PIECES = 4
GROUP = 4


def kernel(
    n,
    lens_hbm,
    acts_hbm,
    grads_hbm,
    win_hbm,
    wout_hbm,
    q_hbm,
    out_hbm,
    lens,
    acts,
    grads,
    win,
    wout,
    qs,
    expand,
    acc,
    stage,
    result,
    out_vmem,
    local_sem,
    acts_sem,
    grads_sem,
    win_sem,
    q_send,
    q_recv,
    row_send,
    row_recv,
    mask_send,
    mask_recv,
    res_send,
    res_recv,
    *per_chunk,
):
    count = len(per_chunk) // 2
    rows, masks = per_chunk[:count], per_chunk[count:]
    me = lax.axis_index("dp")
    n_groups = n // GROUP
    group, lane = me // GROUP, lax.rem(me, GROUP)
    n_half, per_half, _, width = rows[0].shape
    sizes = [ref.shape[2] for ref in rows]
    starts = [sum(sizes[:c]) for c in range(count)]
    ex = stage.shape[1]
    rank = width // 2
    pairs = rank // 2
    half, slot = group // per_half, lax.rem(group, per_half)
    ff = acts.shape[1]
    piece = ff // PIECES

    backward = (group < n_groups - group).astype(jnp.int32)

    def turn(t):
        return t + backward * (n_groups - 2 * t)

    def peer(t):
        t = turn(t)
        return lax.rem(group + t, n_groups) * GROUP + lane

    buddy = me + 1 - 2 * lax.rem(me, 2)
    across = me + 2 - 4 * lax.rem(me // 2, 2)
    across_lane = lax.rem(across, GROUP)

    def start(source, target, sem):
        load = pltpu.make_async_copy(source, target, sem)
        load.start()
        return load

    pieces = [pl.ds(p * piece, piece) for p in range(PIECES)]
    spans = [pl.ds(starts[c], sizes[c]) for c in range(count)]
    load_grads, load_acts = {}, {}

    def fetch_grads(c):
        span = spans[c]
        load_grads[c] = start(grads_hbm.at[span], grads.at[span], grads_sem.at[c])

    def fetch_acts(c, p):
        part = (spans[c], pieces[p])
        load_acts[c, p] = start(acts_hbm.at[*part], acts.at[*part], acts_sem.at[c, p])

    def fetch(c):
        if c < count:
            fetch_grads(c)
            for p in range(PIECES):
                fetch_acts(c, p)

    load_win = []
    for p in range(PIECES):
        part = win.at[:, pieces[p]]
        load_win.append(start(win_hbm.at[:, pieces[p]], part, win_sem.at[p]))
        fetch_acts(0, p)
    load_wout = start(wout_hbm, wout, local_sem.at[1])
    fetch_grads(0)
    load_lens = start(lens_hbm, lens, local_sem.at[3])
    load_q = start(q_hbm, qs.at[lane], local_sem.at[0])
    fetch(1)

    barrier = pltpu.get_barrier_semaphore()
    peers = [peer(t) for t in range(1, n_groups)]
    for other in peers + [buddy, across]:
        pl.semaphore_signal(barrier, inc=1, device_id={"dp": other}, device_id_type=MESH)

    row_copies = []
    for c in range(count):
        span = spans[c]
        total = jnp.zeros((rank, sizes[c]), jnp.float32)
        for p in range(PIECES):
            if c == 0:
                load_win[p].wait()
            load_acts[c, p].wait()
            if p == 0:
                fetch(c + 2)
            total = total + lax.dot_general(
                win[:, pieces[p]], acts[span, pieces[p]], NT, preferred_element_type=jnp.float32
            )
        if c == 0:
            load_wout.wait()
        load_grads[c].wait()
        other = lax.dot_general(wout[...], grads[span], NT, preferred_element_type=jnp.float32)
        both = jnp.concatenate([other, total], axis=0)
        rows[c][half, slot] = both.T.astype(jnp.bfloat16)
        if c == 0:
            load_lens.wait()
            for k in range(count):
                shape = masks[k].shape[1:]
                row_id = lax.broadcasted_iota(jnp.int32, shape, 0) - slot * ex
                lane_id = lax.broadcasted_iota(jnp.int32, shape, 1) - slot * sizes[k]
                inside = (lane_id >= 0) & (lane_id < sizes[k])
                token = lane_id + starts[k]
                first = jnp.int32(0)
                mask = jnp.zeros(shape, jnp.float32)
                for e in range(ex):
                    end = first + lens[0, e]
                    hit = inside & (row_id == e) & (token >= first) & (token < end)
                    mask = jnp.where(hit, 1.0, mask)
                    first = end
                masks[k][group] = mask
            r_id = lax.broadcasted_iota(jnp.int32, (16 * pairs, width), 0)
            c_id = lax.broadcasted_iota(jnp.int32, (16 * pairs, width), 1)
            odd = (r_id >= 8 * pairs).astype(jnp.int32)
            source = 2 * ((r_id - odd * 8 * pairs) // 8) + odd
            expand[...] = jnp.where(source == c_id, 1.0, 0.0).astype(jnp.bfloat16)
            acc[...] = jnp.zeros_like(acc)
            pl.semaphore_wait(barrier, len(peers) + 2)

            load_q.wait()
            q_copies = []
            for i, other in enumerate((across, buddy)):
                copy = pltpu.make_async_remote_copy(
                    src_ref=qs.at[lane],
                    dst_ref=qs.at[lane],
                    send_sem=q_send.at[i],
                    recv_sem=q_recv.at[i],
                    device_id={"dp": other},
                    device_id_type=MESH,
                )
                copy.start()
                q_copies.append(copy)
            mask_copies = []
            for k, t in [(k, t) for k in range(count) for t in range(1, n_groups)]:
                copy = pltpu.make_async_remote_copy(
                    src_ref=masks[k].at[group],
                    dst_ref=masks[k].at[group],
                    send_sem=mask_send.at[turn(t) - 1, k],
                    recv_sem=mask_recv.at[turn(t) - 1, k],
                    device_id={"dp": peer(t)},
                    device_id_type=MESH,
                )
                copy.start()
                mask_copies.append(copy)
        copies = []
        for t in range(1, n_groups):
            copy = pltpu.make_async_remote_copy(
                src_ref=rows[c].at[half, slot],
                dst_ref=rows[c].at[half, slot],
                send_sem=row_send.at[turn(t) - 1, c],
                recv_sem=row_recv.at[turn(t) - 1, c],
                device_id={"dp": peer(t)},
                device_id_type=MESH,
            )
            copy.start()
            copies.append(copy)
        row_copies.append(copies)

    def gather(c):
        for copy in row_copies[c]:
            copy.wait_recv()
        for h in range(n_half):
            block = rows[c][h].reshape(per_half * sizes[c], width)
            mask = masks[c][h * per_half]
            for s in range(1, per_half):
                mask = mask + masks[c][h * per_half + s]
            wide = lax.dot_general(expand[...], block, NT, preferred_element_type=jnp.float32)
            wide = wide.reshape(2 * pairs, 8, mask.shape[1]) * mask[None]
            wide = wide.reshape(16 * pairs, mask.shape[1]).astype(jnp.bfloat16)
            acc[h] += lax.dot_general(wide, block, NN, preferred_element_type=jnp.float32)

    for copy in mask_copies:
        copy.wait_recv()
    for c in range(count - 2):
        gather(c)
    q_copies[0].wait_recv()
    relay = pltpu.make_async_remote_copy(
        src_ref=qs.at[across_lane],
        dst_ref=qs.at[across_lane],
        send_sem=q_send.at[2],
        recv_sem=q_recv.at[2],
        device_id={"dp": buddy},
        device_id_type=MESH,
    )
    relay.start()
    for c in range(count - 2, count):
        gather(c)

    lower = lax.broadcasted_iota(jnp.int32, (8, width), 1) < rank
    columns = []
    for k in range(pairs):
        parts = []
        for h in range(n_half):
            even = pltpu.roll(acc[h, 8 * k : 8 * k + 8], rank, 1)
            odd_rows = acc[h, 8 * pairs + 8 * k : 8 * pairs + 8 * k + 8]
            parts.append(jnp.where(lower, even, odd_rows))
        columns.append(jnp.concatenate(parts, axis=0).astype(jnp.bfloat16))
    example_grads = jnp.concatenate(columns, axis=1)
    q_copies[1].wait_recv()
    relay.wait_recv()
    queries = qs[...].reshape(qs.shape[0] * qs.shape[1], qs.shape[2])
    scores = lax.dot_general(example_grads, queries, NT, preferred_element_type=jnp.float32)
    for s in range(n_groups):
        stage[s] = scores[s * ex : (s + 1) * ex].astype(jnp.bfloat16)
    res_copies = []
    for t in range(1, n_groups):
        copy = pltpu.make_async_remote_copy(
            src_ref=stage.at[lax.rem(group + turn(t), n_groups)],
            dst_ref=result.at[group],
            send_sem=res_send.at[turn(t) - 1],
            recv_sem=res_recv.at[turn(t) - 1],
            device_id={"dp": peer(t)},
            device_id_type=MESH,
        )
        copy.start()
        res_copies.append(copy)
    result[group] = stage[group]
    for copy in res_copies:
        copy.wait_recv()
    cols = qs.shape[0] * qs.shape[1]
    for s in range(n_groups):
        out_vmem[:, s * cols : (s + 1) * cols] = result[s]
    store = pltpu.make_async_copy(out_vmem, out_hbm, local_sem.at[4])
    store.start()
    for copy in q_copies + [relay] + mask_copies + res_copies:
        copy.wait_send()
    for copies in row_copies:
        for copy in copies:
            copy.wait_send()
    store.wait()


def local(n, activations, out_grads, lengths, proj_in, proj_out, queries):
    tokens, ff = activations.shape
    d = out_grads.shape[1]
    rank = proj_in.shape[1]
    ex = lengths.shape[1]
    nq, params = queries.shape
    n_groups = n // GROUP
    per_half = 8 // ex
    n_half = n_groups // per_half
    sizes = [tokens * part // sum(CHUNKS) for part in CHUNKS]
    count = len(sizes)
    width = 2 * rank
    bf16, f32 = jnp.bfloat16, jnp.float32
    dma = pltpu.SemaphoreType.DMA
    others = n_groups - 1
    hbm = pl.BlockSpec(memory_space=pltpu.MemorySpace.HBM)
    return pl.pallas_call(
        functools.partial(kernel, n),
        out_shape=jax.ShapeDtypeStruct((ex, nq * n), bf16),
        in_specs=[hbm] * 6,
        out_specs=pl.BlockSpec(memory_space=pl.ANY),
        scratch_shapes=[
            pltpu.SMEM((1, ex), jnp.int32),
            pltpu.VMEM((tokens, ff), bf16),
            pltpu.VMEM((tokens, d), bf16),
            pltpu.VMEM((rank, ff), bf16),
            pltpu.VMEM((rank, d), bf16),
            pltpu.VMEM((GROUP, nq, params), bf16),
            pltpu.VMEM((8 * rank, width), bf16),
            pltpu.VMEM((n_half, 8 * rank, width), f32),
            pltpu.VMEM((n_groups, ex, GROUP * nq), bf16),
            pltpu.VMEM((n_groups, ex, GROUP * nq), bf16),
            pltpu.VMEM((ex, nq * n), bf16),
            dma((5,)),
            dma((count, PIECES)),
            dma((count,)),
            dma((PIECES,)),
            dma((3,)),
            dma((3,)),
            dma((others, count)),
            dma((others, count)),
            dma((others, count)),
            dma((others, count)),
            dma((others,)),
            dma((others,)),
        ]
        + [pltpu.VMEM((n_half, per_half, size, width), bf16) for size in sizes]
        + [pltpu.VMEM((n_groups, 8, per_half * size), f32) for size in sizes],
        compiler_params=pltpu.CompilerParams(
            collective_id=0, has_side_effects=True, vmem_limit_bytes=56500000
        ),
    )(pltpu.with_memory_space_constraint(lengths, pltpu.HBM), activations, out_grads, proj_in.T, proj_out.T, queries)


def solution(mesh):
    in_specs = (
        P(("parts", "dp"), None),
        P(("parts", "dp"), None),
        P(("parts", "dp"), None),
        P(),
        P(),
        P(("parts", "dp"), None),
    )
    out_specs = P(("parts", "dp"), None)
    body = functools.partial(local, mesh.shape["dp"])
    return jax.shard_map(body, mesh=mesh, in_specs=in_specs, out_specs=out_specs, check_vma=False)
```
